32 devices in a mesh: ens: 4 (over z), shard: 4 (over y, core), tp: 2 (over x).
Axes of the slice: x: 2, y: 2, z: 4, core: 2. Of those that a mesh axis runs over, the one named last changes fastest.
Arguments:
- train_query: bfloat16 [14336, 4096], P(('ens', 'shard'), 'tp'), parts along dimension 0, may hold values from -0.09375 to 0.09375
- low_query: bfloat16 [14336, 32], P(('ens', 'shard')), parts along dimension 0, may hold values from -0.09375 to 0.09375
- high_query: bfloat16 [128, 4096], P('ens', 'tp'), parts along dimension 0, may hold values from -1 to 1
- train_key: bfloat16 [14336, 2048], P(('ens', 'shard'), 'tp'), parts along dimension 0, may hold values from -0.09375 to 0.09375
- low_key: bfloat16 [14336, 32], P(('ens', 'shard')), parts along dimension 0, may hold values from -0.09375 to 0.09375
- high_key: bfloat16 [128, 2048], P('ens', 'tp'), parts along dimension 0, may hold values from -1 to 1
- train_value: bfloat16 [14336, 2048], P(('ens', 'shard'), 'tp'), parts along dimension 0, may hold values from -0.09375 to 0.09375
- low_value: bfloat16 [14336, 32], P(('ens', 'shard')), parts along dimension 0, may hold values from -0.09375 to 0.09375
- high_value: bfloat16 [128, 2048], P('ens', 'tp'), parts along dimension 0, may hold values from -1 to 1
- train_mixed: bfloat16 [16384, 3584], P(('ens', 'tp'), 'shard'), parts along dimension 0, may hold values from -0.09375 to 0.09375
- low_mixed: bfloat16 [16384, 32], P(('ens', 'tp')), parts along dimension 0, may hold values from -0.09375 to 0.09375
- high_mixed: bfloat16 [128, 3584], P('ens', 'shard'), parts along dimension 0, may hold values from -1 to 1
- norm_train: float32 [14336], P(('ens', 'shard', 'tp')), parts along dimension 0, may hold values from 0.25 to 1.75
- norm_step: float32 [14336], P(('ens', 'shard', 'tp')), parts along dimension 0, may hold values from -0.3 to 0.3
Outputs:
- serve_query: bfloat16 [14336, 4096], P('ens', 'tp'), parts along dimension 0
- serve_key: bfloat16 [14336, 2048], P('ens', 'tp'), parts along dimension 0
- serve_value: bfloat16 [14336, 2048], P('ens', 'tp'), parts along dimension 0
- serve_mixed: bfloat16 [16384, 3584], P(('ens', 'tp')), parts along dimension 0
- serve_norm: bfloat16 [14336], P('ens'), parts along dimension 0
The draws below stay inside these ranges and needn't reach their ends.
There are 4 independent parts, one for each index of `ens`. The reference program is written for one: setup_inputs(seed, part) draws one part's arguments, and reference() takes and returns one part's arrays. A program takes and returns all parts, laid end to end along the dimension named above; each array names one. Nothing has to cross between parts.
All inputs are finite; a program needn't handle non-finite values.
Results may differ from the reference program's by a relative error of at most 0.001.
Values may be sent and summed in bfloat16 or wider, within the bound.
A program may use at most 192 MiB of HBM per device.

```python
import jax
import jax.numpy as jnp

D_MODEL = 3584
Q_DIM = 4096
KV_DIM = 2048
RANK = 32


def block_scale(stream_key, shape, split, least, high):
    gain, own = 1.0, jax.random.fold_in(stream_key, 6)
    for dim, parts in split:
        steps = jnp.exp(jax.random.uniform(jax.random.fold_in(own, dim), (parts,), jnp.float32, least / len(split), high / len(split)))
        gain = gain * jnp.repeat(steps, shape[dim] // parts).reshape([-1 if axis == dim else 1 for axis in range(len(shape))])
    return gain


def scatter_about(rng, extent, deviation, most, split=(), held_as=jnp.bfloat16):
    entries = jax.random.normal(rng, extent, jnp.float32) * deviation
    if len(split) > 0:
        entries = block_scale(rng, extent, split, -0.22, 0.18) * entries
    return jnp.clip(entries, min=-most, max=most).astype(held_as)


def setup_inputs(seed: int = 0, part: int = 0) -> dict:
    splits = jax.random.split(jax.random.key(seed), 15)
    own_keys = jax.random.split(jax.random.fold_in(splits[14], part), 15)
    train_query = scatter_about(own_keys[0], (D_MODEL, Q_DIM), D_MODEL ** -0.5, 0.09375, ((0, 4), (1, 2)))
    low_query = scatter_about(own_keys[1], (D_MODEL, RANK), D_MODEL ** -0.5, 0.09375, ((0, 4),))
    high_query = scatter_about(own_keys[2], (RANK, Q_DIM), RANK ** -0.5, 1.0, ((1, 2),))
    train_key = scatter_about(own_keys[3], (D_MODEL, KV_DIM), D_MODEL ** -0.5, 0.09375, ((0, 4), (1, 2)))
    low_key = scatter_about(own_keys[4], (D_MODEL, RANK), D_MODEL ** -0.5, 0.09375, ((0, 4),))
    high_key = scatter_about(own_keys[5], (RANK, KV_DIM), RANK ** -0.5, 1.0, ((1, 2),))
    train_value = scatter_about(own_keys[6], (D_MODEL, KV_DIM), D_MODEL ** -0.5, 0.09375, ((0, 4), (1, 2)))
    low_value = scatter_about(own_keys[7], (D_MODEL, RANK), D_MODEL ** -0.5, 0.09375, ((0, 4),))
    high_value = scatter_about(own_keys[8], (RANK, KV_DIM), RANK ** -0.5, 1.0, ((1, 2),))
    train_mixed = scatter_about(own_keys[9], (Q_DIM, D_MODEL), Q_DIM ** -0.5, 0.09375, ((0, 2), (1, 4)))
    low_mixed = scatter_about(own_keys[10], (Q_DIM, RANK), Q_DIM ** -0.5, 0.09375, ((0, 2),))
    high_mixed = scatter_about(own_keys[11], (RANK, D_MODEL), RANK ** -0.5, 1.0, ((1, 4),))
    norm_train = jnp.clip(1.0 + 0.15 * jax.random.normal(own_keys[12], (D_MODEL,), jnp.float32), 0.25, 1.75)
    norm_step = jnp.clip(jax.random.uniform(own_keys[13], (D_MODEL,), jnp.float32, -0.3, 0.3) * block_scale(own_keys[13], (D_MODEL,), ((0, 8),), -0.4, 0.0), -0.3, 0.3)
    return {"train_query": train_query, "low_query": low_query, "high_query": high_query, "train_key": train_key, "low_key": low_key, "high_key": high_key, "train_value": train_value, "low_value": low_value, "high_value": high_value, "train_mixed": train_mixed, "low_mixed": low_mixed, "high_mixed": high_mixed, "norm_train": norm_train, "norm_step": norm_step}


mix_rate = 1.0


def reference(train_query, low_query, high_query, train_key, low_key, high_key, train_value, low_value, high_value, train_mixed, low_mixed, high_mixed, norm_train, norm_step):
    fresh_query = train_query.astype(jnp.float32) + mix_rate * jnp.dot(low_query, high_query, preferred_element_type=jnp.float32)
    fresh_key = train_key.astype(jnp.float32) + mix_rate * jnp.dot(low_key, high_key, preferred_element_type=jnp.float32)
    fresh_value = train_value.astype(jnp.float32) + mix_rate * jnp.dot(low_value, high_value, preferred_element_type=jnp.float32)
    fresh_mixed = train_mixed.astype(jnp.float32) + mix_rate * jnp.dot(low_mixed, high_mixed, preferred_element_type=jnp.float32)
    serve_query = fresh_query.astype(jnp.bfloat16)
    serve_key = fresh_key.astype(jnp.bfloat16)
    serve_value = fresh_value.astype(jnp.bfloat16)
    serve_mixed = fresh_mixed.astype(jnp.bfloat16)
    serve_norm = (norm_train + norm_step).astype(jnp.bfloat16)
    return serve_query, serve_key, serve_value, serve_mixed, serve_norm
```

```python
import functools

import jax
import jax.numpy as jnp
from jax import lax
from jax.experimental import pallas as pl
from jax.experimental.pallas import tpu as pltpu
from jax.sharding import PartitionSpec as P


mix_rate = 1.0
UNIT = 128

PLAN = (
    ("key", 0, 1),
    ("key", 1, 7),
    ("query", 0, 4),
    ("query", 4, 7),
    ("value", 0, 7),
    ("mixed", 0, 8),
    ("mixed", 8, 14),
    ("mixed", 14, 16),
)


def merged(train, low, high):
    fresh = train.astype(jnp.float32) + mix_rate * jnp.dot(low, high, preferred_element_type=jnp.float32)
    return fresh.astype(jnp.bfloat16)


def merge_kernel(train_ref, turned_ref, high_ref, out_ref):
    update = lax.dot_general(
        turned_ref[...], high_ref[...], (((0,), (0,)), ((), ())), preferred_element_type=jnp.float32
    )
    out_ref[...] = (train_ref[...].astype(jnp.float32) + mix_rate * update).astype(out_ref.dtype)


def merge_piece(train, turned, high, first, last):
    columns, rank = train.shape[1], turned.shape[0]
    rows = (last - first) * UNIT
    return pl.pallas_call(
        merge_kernel,
        grid=(last - first,),
        in_specs=[
            pl.BlockSpec((UNIT, columns), lambda i: (first + i, 0)),
            pl.BlockSpec((rank, UNIT), lambda i: (0, first + i)),
            pl.BlockSpec((rank, columns), lambda i: (0, 0)),
        ],
        out_specs=pl.BlockSpec((UNIT, columns), lambda i: (i, 0)),
        out_shape=jax.ShapeDtypeStruct((rows, columns), jnp.bfloat16),
        cost_estimate=pl.CostEstimate(
            flops=2 * rows * columns * rank, bytes_accessed=4 * rows * columns, transcendentals=0
        ),
        name="merge",
    )(train, turned, high)


def place_kernel(masks, row, by_rows, aliased, *refs):
    n = len(masks)
    sources = refs[:n]
    out_ref, staged, in_sems, out_sems = refs[n + aliased :]
    rows, columns = sources[0].shape
    me = lax.axis_index("shard")
    loads = []
    for j in range(n):
        load = pltpu.make_async_copy(sources[j], staged.at[j], in_sems.at[j])
        load.start()
        loads.append(load)
    stores = []
    for j, mask in enumerate(masks):
        low, high = me % 2, me // 2
        owner = (high + mask // 2 - 2 * high * (mask // 2)) * 2 + (low + mask % 2 - 2 * low * (mask % 2))
        if by_rows:
            span = out_ref.shape[0] // 4
            target = out_ref.at[pl.ds(pl.multiple_of(owner * span + row, UNIT), rows), :]
        else:
            target = out_ref.at[pl.ds(row, rows), pl.ds(pl.multiple_of(owner * columns, 128), columns)]
        store = pltpu.make_async_copy(staged.at[j], target, out_sems.at[j])
        loads[j].wait()
        store.start()
        stores.append(store)
    for store in stores:
        store.wait()


def place(out, out_shape, pieces, row, by_rows):
    masks = tuple(mask for mask, _ in pieces)
    arrays = [array for _, array in pieces]
    n = len(arrays)
    rows, columns = arrays[0].shape
    aliased = out is not None
    return pl.pallas_call(
        functools.partial(place_kernel, masks, row, by_rows, aliased),
        in_specs=[pl.BlockSpec(memory_space=pltpu.HBM)] * (n + aliased),
        out_specs=pl.BlockSpec(memory_space=pltpu.HBM),
        out_shape=out_shape,
        scratch_shapes=[
            pltpu.VMEM((n, rows, columns), jnp.bfloat16),
            pltpu.SemaphoreType.DMA((n,)),
            pltpu.SemaphoreType.DMA((n,)),
        ],
        input_output_aliases={n: 0} if aliased else {},
        cost_estimate=pl.CostEstimate(flops=0, bytes_accessed=4 * n * rows * columns, transcendentals=0),
        name="place",
    )(*arrays, *([out] if aliased else []))


def swap(array, mask):
    return lax.ppermute(array, "shard", [(s, s ^ mask) for s in range(4)])


def gathered_norm(norm_train, norm_step):
    fresh = (norm_train + norm_step).astype(jnp.bfloat16)
    return lax.all_gather(fresh, ("shard", "tp"), axis=0, tiled=True)


def after(array, earlier):
    return lax.optimization_barrier((array, earlier))[0]


def exchange(weights, norm_train, norm_step):
    turned = {name: low.T for name, (_, low, _, _) in weights.items()}
    shapes = {
        name: jax.ShapeDtypeStruct(
            (train.shape[0] * (4 if by_rows else 1), train.shape[1] * (1 if by_rows else 4)), jnp.bfloat16
        )
        for name, (train, _, _, by_rows) in weights.items()
    }
    outs = {name: None for name in weights}
    own, across, beside, both = [], [], [], []
    for k, (name, first, last) in enumerate(PLAN):
        train, _, high, _ = weights[name]
        own.append(merge_piece(train, turned[name], high, first, last))
        across.append(swap(own[k], 2))
        beside.append(swap(own[k], 1))
    serve_norm = gathered_norm(after(norm_train, own[-1]), norm_step)
    across[1] = after(across[1], serve_norm)
    for k in range(len(PLAN)):
        both.append(swap(across[k], 1))
    for pieces in (
        [((0, own[k]), (1, beside[k])) for k in range(len(PLAN))],
        [((2, across[k]), (3, both[k])) for k in range(len(PLAN))],
    ):
        for k, (name, first, _) in enumerate(PLAN):
            outs[name] = place(outs[name], shapes[name], pieces[k], first * UNIT, weights[name][3])
    return outs, serve_norm


def per_device(
    fits,
    train_query,
    low_query,
    high_query,
    train_key,
    low_key,
    high_key,
    train_value,
    low_value,
    high_value,
    train_mixed,
    low_mixed,
    high_mixed,
    norm_train,
    norm_step,
):
    weights = {
        "query": (train_query, low_query, high_query, True),
        "key": (train_key, low_key, high_key, True),
        "value": (train_value, low_value, high_value, True),
        "mixed": (train_mixed, low_mixed, high_mixed, False),
    }
    if fits:
        outs, serve_norm = exchange(weights, norm_train, norm_step)
    else:
        serve_norm = gathered_norm(norm_train, norm_step)
        outs = {
            name: lax.all_gather(merged(train, low, high), "shard", axis=0 if by_rows else 1, tiled=True)
            for name, (train, low, high, by_rows) in weights.items()
        }
    return (outs["query"], outs["key"], outs["value"], outs["mixed"], serve_norm)


def solution(mesh):
    fits = mesh.shape["shard"] == 4 and mesh.shape["tp"] == 2
    return jax.shard_map(
        functools.partial(per_device, fits),
        mesh=mesh,
        in_specs=(
            P(("ens", "shard"), "tp"),
            P(("ens", "shard"), None),
            P("ens", "tp"),
            P(("ens", "shard"), "tp"),
            P(("ens", "shard"), None),
            P("ens", "tp"),
            P(("ens", "shard"), "tp"),
            P(("ens", "shard"), None),
            P("ens", "tp"),
            P(("ens", "tp"), "shard"),
            P(("ens", "tp"), None),
            P("ens", "shard"),
            P(("ens", "shard", "tp")),
            P(("ens", "shard", "tp")),
        ),
        out_specs=(
            P("ens", "tp"),
            P("ens", "tp"),
            P("ens", "tp"),
            P(("ens", "tp"), None),
            P("ens"),
        ),
        check_vma=False,
    )
```
